256 devices in a mesh: chan: 64 (over x, y, z_hi, core), tm: 4 (over z_lo).
Axes of the slice: x: 4, y: 4, z: 8 (z_hi: 2, z_lo: 4; z = z_hi * 4 + z_lo), core: 2. Of those that a mesh axis runs over, the one named last changes fastest.
Arguments:
- voltages: bfloat16 [2, 64, 2048, 512], P(None, None, 'chan', 'tm'), may hold values from -0.25 to 0.25
- assignment: int32 [1024, 1], replicated, may hold values from 0 to 7; in each aligned block of 1024 rows (0 to 1023, 1024 to 2047, ...) at most 192 rows name the same one
- slot_subarray_index: int32 [8], replicated, may hold values from 0 to 7, each once
Outputs:
- visibilities: float32 [8, 64, 2, 384, 384], P('tm', 'chan')
The draws below stay inside these ranges and needn't reach their ends.
Inputs may be any that keep to these rules, and one draw needn't show every extreme that they name: `assignment`: no subarray holds more than 192 antennas; one holds exactly 192. `slot_subarray_index`: each subarray appears once.
All inputs are finite; a program needn't handle non-finite values.
Results may differ from the reference program's by a relative error of at most 0.008.
Values may be sent and summed in bfloat16 or wider, within the bound.
A program may use at most 64 MiB of HBM per device.

```python
import math
import jax
import jax.numpy as jnp
import numpy as np
from jax import lax

ANTENNA_TOTAL = 1024
SUBARRAY_TOTAL = 8
SAMPLES_LOCAL = 128
INPUTS = 2048
ANTENNA_LIMIT = 192
SLOT = 384
CHANS = 64
SAMPLES = 512
N_TM = 4


def steps_of(key, dims, shards, low, high):
    gain = 1.0
    for axis_at, shards_of in shards:
        steps = jax.random.uniform(jax.random.fold_in(jax.random.fold_in(key, 6), axis_at), (shards_of,), jnp.float32, low / len(shards), high / len(shards))
        gain = gain * jnp.repeat(jnp.exp(steps), dims[axis_at] // shards_of).reshape((-1,) + (1,) * (len(dims) - 1 - axis_at))
    return gain


def deal_out(stream_key, own, number, rows, count, top, bound, slope):
    order = jax.random.permutation(stream_key, count)
    crowded, ordinary = shares(count, rows * top, bound, slope, True), shares(count, rows * top, bound, slope, False)
    places = jnp.arange(count)

    def named(tallies, offset_by):
        used = int((tallies > 0).sum())
        fixed = max(1, used // 4)
        shifted = fixed + (places - fixed + offset_by * (used - fixed)) % max(1, count - fixed)
        return jnp.zeros((count,), jnp.int32).at[order[jnp.where(places < fixed, places, shifted)]].set(jnp.asarray(tallies, jnp.int32))

    tallies = jnp.where(number % 4 == 0, named(crowded, number // 4), named(ordinary, number - number // 4 - 1))
    mixed = jax.random.permutation(jax.random.fold_in(own, 3), count)
    giver, receiver = mixed[0:count // 2 * 2:2], mixed[1:count // 2 * 2:2]
    margin = jnp.minimum(tallies[giver] - 1, bound - tallies[receiver]) // 2
    margin = jnp.where((giver == order[0]) | (receiver == order[0]) | (tallies[receiver] == 0), 0, jnp.maximum(margin, 0))
    shifted = jax.random.randint(jax.random.fold_in(own, 4), (count // 2,), 0, 1 << 20) % (margin + 1)
    tallies = tallies.at[giver].add(-shifted).at[receiver].add(shifted)
    labels = jnp.searchsorted(jnp.cumsum(tallies), jnp.arange(rows * top), side="right").astype(jnp.int32)
    grid = labels.reshape(top, rows).T
    grid = grid[jax.random.permutation(jax.random.fold_in(own, 1), rows)]
    offset_by = jax.random.randint(jax.random.fold_in(own, 2), (rows, 1), 0, top)
    return jnp.take_along_axis(grid, (jnp.arange(top)[None, :] + offset_by) % top, axis=1)


def shares(number_of, total, limit, lean, full):
    weights = [(1 << 20) // math.isqrt(rank ** lean) + 1 for rank in range(1, number_of + 1)]
    largest = limit if full else min(limit, max(-(-total // number_of), total * weights[0] // sum(weights)))
    least = 1 if total - largest >= number_of - 1 else 0
    holding, spare = [largest] + [least] * (number_of - 1), total - largest - least * (number_of - 1)
    while spare > 0:
        free = [i for i in range(1, number_of) if holding[i] < largest] or [i for i in range(1, number_of) if holding[i] < limit]
        mass, remaining = sum([weights[i] for i in free]), spare
        for i in free:
            addition = min(limit - holding[i], max(1, remaining * weights[i] // mass), spare)
            holding[i] = holding[i] + addition
            spare = spare - addition
    return np.array(holding)


def scatter_about(rng, shape, scale, limit, pieces=(), kind=jnp.bfloat16):
    array = jax.random.normal(rng, shape, jnp.float32) * scale
    if len(pieces) > 0:
        array = steps_of(rng, shape, pieces, -0.22, 0.18) * array
    return jnp.clip(array, min=-limit, max=limit).astype(kind)


def setup_inputs(seed: int = 0) -> dict:
    seeds = jax.random.split(jax.random.key(seed), 4)
    voltages = scatter_about(seeds[0], (2, CHANS, INPUTS, SAMPLES), SAMPLES ** -0.5, 0.25, ((2, 64), (3, 4)))
    assignment_keys = jax.random.split(jax.random.fold_in(seeds[1], 1), ANTENNA_TOTAL // ANTENNA_TOTAL)
    assignment_turns = jax.random.permutation(jax.random.fold_in(seeds[1], 3), ANTENNA_TOTAL // ANTENNA_TOTAL)
    assignment = jax.vmap(lambda own, number: deal_out(jax.random.fold_in(seeds[1], 2), own, number, ANTENNA_TOTAL, SUBARRAY_TOTAL, 1, ANTENNA_LIMIT, 2))(assignment_keys, assignment_turns).reshape((ANTENNA_TOTAL, 1))
    slot_subarray_index = jax.random.permutation(seeds[2], SUBARRAY_TOTAL).astype(jnp.int32)
    return {"voltages": voltages, "assignment": assignment, "slot_subarray_index": slot_subarray_index}


def result_slot_lookup(assignment, slot_subarray_index):
    owner = jnp.repeat(assignment[:, 0], 2).astype(jnp.int32)
    onehot = (owner[:, None] == jnp.arange(SUBARRAY_TOTAL, dtype=jnp.int32)[None, :]).astype(jnp.int32)
    ranks = jnp.sum((jnp.cumsum(onehot, axis=0) - onehot) * onehot, axis=1).astype(jnp.int32)
    table = jnp.full((SUBARRAY_TOTAL, SLOT), INPUTS, jnp.int32)
    table = table.at[owner, ranks].set(jnp.arange(INPUTS, dtype=jnp.int32))
    return table[slot_subarray_index.astype(jnp.int32)].reshape(-1).astype(jnp.int32)


def compact(block, rows):
    parts, chans, inputs, samples = block.shape
    padded_voltages = jnp.concatenate([block, jnp.zeros((parts, chans, 1, samples), block.dtype)], axis=2)
    picked = jnp.take(padded_voltages, rows, axis=2)
    picked = picked.reshape(parts, chans, SUBARRAY_TOTAL, SLOT, samples)
    picked = jnp.transpose(picked, (2, 1, 0, 3, 4))
    return picked.reshape(SUBARRAY_TOTAL, chans, 2 * SLOT, samples)


def gram(stacked):
    stacked = stacked.astype(jnp.float32)
    full = jnp.einsum("...pt,...qt->...pq", stacked, stacked)
    half = stacked.shape[-2] // 2
    real = full[..., :half, :half] + full[..., half:, half:]
    imag = full[..., half:, :half] - full[..., :half, half:]
    return jnp.stack([real, imag], axis=-3)


def blocked_gram(stacked):
    total = None
    for block_index in range(N_TM):
        piece = stacked[..., block_index * SAMPLES_LOCAL:(block_index + 1) * SAMPLES_LOCAL]
        rounded = gram(piece).astype(jnp.bfloat16)
        rounded = lax.optimization_barrier(rounded).astype(jnp.float32)
        total = rounded if total is None else total + rounded
    return total


def reference(voltages, assignment, slot_subarray_index):
    rows = result_slot_lookup(assignment, slot_subarray_index)

    def one_channel(block):
        return blocked_gram(compact(block[:, None], rows))[:, 0]

    result = lax.map(one_channel, jnp.moveaxis(voltages, 1, 0))
    return jnp.transpose(result, (1, 0, 2, 3, 4))
```

```python
import functools

import jax
import jax.numpy as jnp
from jax import lax
from jax.experimental import pallas as pl
from jax.experimental.pallas import tpu as pltpu
from jax.sharding import PartitionSpec as P

SLOT = 384
LEVELS = (352, 400, 768)
CHUNKS = ((1, 0), (1, 1), (0, 0), (0, 1))
PEERS = 32
BF = jnp.bfloat16
MESH = pl.DeviceIdType.MESH
NT = (((1,), (1,)), ((), ()))
VMEM = pl.BlockSpec(memory_space=pltpu.VMEM)
SMEM = pl.BlockSpec(memory_space=pltpu.SMEM)
ANY = pl.BlockSpec(memory_space=pl.ANY)


def exact_dot(a, b):
    return jnp.dot(a, b, precision=lax.Precision.HIGHEST, preferred_element_type=jnp.float32)


def iota(shape, dim):
    return lax.broadcasted_iota(jnp.int32, shape, dim)


def slots_of(assigned, index_ref):
    slot = jnp.zeros_like(assigned)
    for s in range(8):
        slot = jnp.where(assigned == index_ref[s], s, slot)
    return slot


def level_kernel(assigned_ref, index_ref, level_ref):
    pair = slots_of(assigned_ref[...], index_ref) >> 1
    half = (iota((8, 128), 1) >> 5) & 1
    most = jnp.int32(0)
    for g in range(4):
        for h in range(2):
            most = jnp.maximum(most, jnp.sum(jnp.where((pair == g) & (half == h), 2, 0)))
    level = jnp.int32(0)
    for rows in LEVELS[:-1]:
        level = level + jnp.where(most > rows, 1, 0)
    level_ref[0] = level


def spread(values, half):
    source, target = iota((128, 128), 0), iota((128, 128), 1)
    pick = source == (target >> 6) * 64 + half * 32 + ((target & 63) >> 1)
    return exact_dot(values.astype(jnp.float32), pick.astype(jnp.float32)).astype(jnp.int32)


def counts_before(mask, same):
    ones = mask.astype(jnp.float32)
    source, target = iota((128, 128), 0), iota((128, 128), 1)
    within = exact_dot(ones, (same & (source < target)).astype(jnp.float32))
    totals = exact_dot(ones, same.astype(jnp.float32))
    offset = jnp.zeros((1, 128), jnp.float32)
    rows = []
    for b in range(8):
        rows.append(offset)
        offset = offset + totals[b : b + 1]
    return (within + jnp.concatenate(rows, axis=0)).astype(jnp.int32)


def correlate(
    K, assigned_ref, index_ref, v_ref, out_ref, v, buf, select, merge, stage, recv, z, result,
    v_sem, send1, recv1, send2, recv2, out_sem,
):
    chan, t = lax.axis_index("chan"), lax.axis_index("tm")
    xy, h, core = chan // 4, (chan // 2) % 2, chan % 2
    me, depth = xy * 2 + core, h * 4 + t

    def group(j):
        p = (me + j) % PEERS
        return p // 2, p % 2, {"chan": ((p // 2) * 2 + h) * 2 + p % 2, "tm": t}

    def column(half, row):
        return {"chan": (xy * 2 + half) * 2 + core, "tm": row}

    load = pltpu.make_async_copy(v_ref, v, v_sem)
    load.start()
    barrier = pltpu.get_barrier_semaphore()

    def greet(j, carry):
        pl.semaphore_signal(barrier, inc=1, device_id=group(j)[2], device_id_type=MESH)
        return carry

    lax.fori_loop(1, PEERS, greet, 0)
    for o in range(8):
        half, row = ((h + o // 4) % 2), (t + o) % 4
        if o:
            pl.semaphore_signal(barrier, inc=1, device_id=column(half, row), device_id_type=MESH)

    load.wait()
    pl.semaphore_wait(barrier, PEERS - 1 + 7)

    def first(i, j):
        away, part = CHUNKS[i]
        there, there_core, device = group(j)
        ch = (h + away) % 2
        return pltpu.make_async_remote_copy(
            v.at[part, there, ch, there_core], buf.at[i, me], send1.at[i, j], recv1.at[i, j],
            device_id=device, device_id_type=MESH,
        )

    for i, (away, part) in enumerate(CHUNKS):
        lax.fori_loop(1, PEERS, lambda j, c, i=i: (first(i, j).start(), c)[1], 0)
        buf[i, me] = v[part, xy, (h + away) % 2, core]

    lane = iota((8, 128), 1)
    slot = slots_of(assigned_ref[...], index_ref)
    pair = slot >> 1
    source, target = iota((128, 128), 0), iota((128, 128), 1)
    same = ((source >> 5) & 1) == ((target >> 5) & 1)
    place = jnp.zeros((8, 128), jnp.int32)
    for g in range(4):
        place = jnp.where(pair == g, counts_before(pair == g, same), place)
    final = jnp.zeros((8, 128), jnp.int32)
    for s in range(2):
        mine = slot == 2 * t + s
        final = jnp.where(mine, s * SLOT + 2 * counts_before(mine, source >= 0), final)
    pol = lane & 1

    goal = spread(pair, h) * K + pol * (K // 2) + spread(place, h)
    tall = iota((K, 128), 0)
    for g in range(4):
        for b in range(8):
            hit = tall == goal[b : b + 1] - g * K
            select[g, :, b * 128 : (b + 1) * 128] = jnp.where(hit, 1.0, 0.0).astype(BF)
    sub = iota((8, 128), 0)
    for half in range(2):
        here = jnp.where(spread(pair, half) == t, pol * (K // 2) + spread(place, half), -1)
        row = spread(final, half) + pol
        found = jnp.zeros((8, K), jnp.float32)
        for b in range(8):
            hit = jnp.where(tall == here[b : b + 1], 1.0, 0.0).astype(BF)
            known = jnp.where(
                sub == 0, row[b : b + 1] >> 8, jnp.where(sub == 1, row[b : b + 1] & 255, jnp.where(sub == 2, 1, 0))
            )
            found = found + lax.dot_general(
                known.astype(jnp.float32).astype(BF), hit, NT, preferred_element_type=jnp.float32
            )
        at = jnp.where(found[2:3] > 0.5, 256.0 * found[0:1] + found[1:2], -1.0).astype(jnp.int32)
        merge[half] = jnp.where(iota((2 * SLOT, K), 0) == at, 1.0, 0.0).astype(BF)

    def second(i, o):
        away, part = CHUNKS[i]
        row = (t + o) % 4
        return pltpu.make_async_remote_copy(
            stage.at[i, row], recv.at[part, depth], send2.at[i, o], recv2.at[part, depth],
            device_id=column((h + away) % 2, row), device_id_type=MESH,
        )

    for i, (away, part) in enumerate(CHUNKS):
        lax.fori_loop(1, PEERS, lambda j, c, i=i: (first(i, j).wait_recv(), c)[1], 0)
        rows = buf[i].reshape(PEERS * 32, 128)
        for o in range(4):
            row = (t + o) % 4
            packed = jnp.dot(select[row], rows, preferred_element_type=jnp.float32).astype(BF)
            if away == 0 and o == 0:
                recv[part, depth] = packed
            else:
                stage[i, row] = packed
                second(i, o).start()

    def arrived(part, o):
        half, row = (h + o // 4) % 2, (t + o) % 4
        return pltpu.make_async_remote_copy(
            stage.at[0, 0], recv.at[part, half * 4 + row], send2.at[0, 0], recv2.at[part, half * 4 + row],
            device_id=column(half, row), device_id_type=MESH,
        )

    for part in range(2):
        for o in range(1, 8):
            arrived(part, o).wait_recv()
        total = jnp.zeros((2 * SLOT, 512), jnp.float32)
        for half in range(2):
            wide = jnp.concatenate([recv[part, half * 4 + b] for b in range(4)], axis=1)
            total = total + jnp.dot(merge[half], wide, preferred_element_type=jnp.float32)
        z[part] = total.astype(BF)

    def times(a, b):
        return lax.dot_general(a, b, NT, preferred_element_type=jnp.float32)

    stores = []
    for s in range(2):
        re, im = z[0, s * SLOT : (s + 1) * SLOT], z[1, s * SLOT : (s + 1) * SLOT]
        for k in range(2):
            result[s, k] = times(re, re) + times(im, im) if k == 0 else times(im, re) - times(re, im)
            store = pltpu.make_async_copy(result.at[s, k], out_ref.at[s, 0, k], out_sem.at[s, k])
            store.start()
            stores.append(store)
    for i, (away, part) in enumerate(CHUNKS):
        lax.fori_loop(1, PEERS, lambda j, c, i=i: (first(i, j).wait_send(), c)[1], 0)
        for o in range(4):
            if away or o:
                second(i, o).wait_send()
    for store in stores:
        store.wait()


def correlator(number, K):
    def call(voltages, assigned, index):
        return pl.pallas_call(
            functools.partial(correlate, K),
            out_shape=jax.ShapeDtypeStruct((2, 1, 2, SLOT, SLOT), jnp.float32),
            in_specs=[VMEM, SMEM, ANY],
            out_specs=ANY,
            scratch_shapes=[
                pltpu.VMEM((2, 16, 2, 2, 32, 128), BF),
                pltpu.VMEM((4, PEERS, 32, 128), BF),
                pltpu.VMEM((4, K, 1024), BF),
                pltpu.VMEM((2, 2 * SLOT, K), BF),
                pltpu.VMEM((4, 4, K, 128), BF),
                pltpu.VMEM((2, 8, K, 128), BF),
                pltpu.VMEM((2, 2 * SLOT, 512), BF),
                pltpu.VMEM((2, 2, SLOT, SLOT), jnp.float32),
                pltpu.SemaphoreType.DMA,
                pltpu.SemaphoreType.DMA((4, PEERS)),
                pltpu.SemaphoreType.DMA((4, PEERS)),
                pltpu.SemaphoreType.DMA((4, 4)),
                pltpu.SemaphoreType.DMA((2, 8)),
                pltpu.SemaphoreType.DMA((2, 2)),
            ],
            compiler_params=pltpu.CompilerParams(
                collective_id=number, has_side_effects=True, vmem_limit_bytes=48 << 20
            ),
            name=f"correlate_{K}",
        )(assigned, index, voltages)

    return call


def shards(voltages, assignment, slot_subarray_index):
    assigned = assignment.reshape(8, 128)
    level = pl.pallas_call(
        level_kernel,
        out_shape=jax.ShapeDtypeStruct((1,), jnp.int32),
        in_specs=[VMEM, SMEM],
        out_specs=SMEM,
        name="level",
    )(assigned, slot_subarray_index)
    branches = [correlator(number, K) for number, K in enumerate(LEVELS)]
    voltages = voltages.reshape(2, 16, 2, 2, 32, 128)
    return lax.switch(level[0], branches, voltages, assigned, slot_subarray_index)


def solution(mesh):
    placed = (P(None, None, "chan", "tm"), P(), P())
    return jax.shard_map(
        shards,
        mesh=mesh,
        in_specs=placed,
        out_specs=P("tm", "chan", None, None, None),
        check_vma=False,
    )
```

```python
import functools

import jax
import jax.numpy as jnp
from jax import lax
from jax.experimental import pallas as pl
from jax.experimental.pallas import tpu as pltpu
from jax.sharding import PartitionSpec as P

SLOT = 384
LEVELS = (304, 320, 336, 352, 368, 384, 400, 432, 768)
PEERS = 32
SELF = 20
BF = jnp.bfloat16
MESH = pl.DeviceIdType.MESH
NT = (((1,), (1,)), ((), ()))
VMEM = pl.BlockSpec(memory_space=pltpu.VMEM)
SMEM = pl.BlockSpec(memory_space=pltpu.SMEM)
ANY = pl.BlockSpec(memory_space=pl.ANY)


def count_dot(a, b):
    return jnp.dot(as_bf16(a), as_bf16(b), preferred_element_type=jnp.float32)


def as_bf16(values):
    return values.astype(jnp.float32).astype(BF)


def iota(shape, dim):
    return lax.broadcasted_iota(jnp.int32, shape, dim)


def slots_of(assigned, index_ref):
    slot = jnp.zeros_like(assigned)
    for s in range(8):
        slot = jnp.where(assigned == index_ref[s], s, slot)
    return slot


def level_kernel(assigned_ref, index_ref, level_ref):
    pair = slots_of(assigned_ref[...], index_ref) >> 1
    half = (iota((8, 128), 1) >> 5) & 1
    most = jnp.int32(0)
    for g in range(4):
        for h in range(2):
            most = jnp.maximum(most, jnp.sum(jnp.where((pair == g) & (half == h), 2, 0)))
    level = jnp.int32(0)
    for rows in LEVELS[:-1]:
        level = level + jnp.where(most > rows, 1, 0)
    level_ref[0] = level


def counts_before(masks, same, before):
    n = len(masks)
    found = count_dot(jnp.concatenate(masks, axis=0), jnp.concatenate([same & before, same], axis=1))
    sub, other = iota((8 * n, 8 * n), 0), iota((8 * n, 8 * n), 1)
    earlier = ((sub >> 3) == (other >> 3)) & (sub > other)
    total = (found[:, :128] + count_dot(earlier, found[:, 128:])).astype(jnp.int32)
    return [total[8 * i : 8 * i + 8] for i in range(n)]


def to_rows(values, half):
    source, target = iota((128, 128), 0), iota((128, 128), 1)
    pick = source == (target >> 6) * 64 + half * 32 + ((target & 63) >> 1)
    moved = count_dot(jnp.concatenate(values, axis=0), pick).astype(jnp.int32)
    return [moved[8 * i : 8 * i + 8] for i in range(len(values))]


def correlate(
    K, assigned_ref, index_ref, v_ref, z, v, buf, select, merge, stage, recv, notes,
    v_sem, send1, recv1, send2, recv2,
):
    chan, t = lax.axis_index("chan"), lax.axis_index("tm")
    xy, h, core = chan // 4, (chan // 2) % 2, chan % 2
    me, depth = xy * 2 + core, h * 4 + t

    def group(j):
        there, there_core = ((xy // 4 + 2 + j // 8) % 4) * 4 + (xy + 2 + (j // 2) % 4) % 4, (core + j) % 2
        return there, there_core, {"chan": (there * 2 + h) * 2 + there_core, "tm": t}

    def others(act):
        def step(j, carry):
            act(j)
            return carry

        lax.fori_loop(0, SELF, step, 0)
        lax.fori_loop(SELF + 1, PEERS, step, 0)

    def column(half, row):
        return {"chan": (xy * 2 + half) * 2 + core, "tm": row}

    load = pltpu.make_async_copy(v_ref, v, v_sem)
    load.start()
    barrier = pltpu.get_barrier_semaphore()

    others(lambda j: pl.semaphore_signal(barrier, inc=1, device_id=group(j)[2], device_id_type=MESH))
    for o in range(1, 8):
        pl.semaphore_signal(
            barrier, inc=1, device_id=column((h + o // 4) % 2, (t + o) % 4), device_id_type=MESH
        )

    slot = slots_of(assigned_ref[...], index_ref)
    pair = slot >> 1
    source, target = iota((128, 128), 0), iota((128, 128), 1)
    same, before = ((source >> 5) & 1) == ((target >> 5) & 1), source < target
    counts = counts_before([pair == g for g in range(4)], same, before)
    place = sum(jnp.where(pair == g, counts[g], 0) for g in range(4))
    pol = iota((8, 128), 1) & 1
    pairs, high, low = to_rows([pair, place >> 4, place & 15], h)
    notes[0] = pairs * K + pol * (K // 2) + high * 16 + low

    load.wait()
    pl.semaphore_wait(barrier, PEERS - 1 + 7)

    def first(away, part, j):
        there, there_core, device = group(j)
        i = 2 * (1 - away) + part
        return pltpu.make_async_remote_copy(
            v.at[part, there, (h + away) % 2, there_core], buf.at[i, me], send1.at[i, j], recv1.at[i, j],
            device_id=device, device_id_type=MESH,
        )

    def chunks(act):
        for away in (1, 0):

            def step(part, carry, away=away):
                act(away, part)
                return carry

            lax.fori_loop(0, 2, step, 0)

    def start(away, part):
        others(lambda j: first(away, part, j).start())
        buf[2 * (1 - away) + part, me] = v[part, xy, (h + away) % 2, core]

    chunks(start)

    tall = iota((K, 128), 0)

    def pick(g, carry):
        for b in range(8):
            hit = tall == notes[0, b : b + 1] - g * K
            select[g, :, b * 128 : (b + 1) * 128] = jnp.where(hit, 1.0, 0.0).astype(BF)
        return carry

    lax.fori_loop(0, 4, pick, 0)

    def second(away, part, o):
        i, row = 2 * (1 - away) + part, (t + o) % 4
        return pltpu.make_async_remote_copy(
            stage.at[i, row], recv.at[part, t, pl.ds(h * K, K)], send2.at[i, o], recv2.at[part, depth],
            device_id=column((h + away) % 2, row), device_id_type=MESH,
        )

    def pack(away, part):
        i = 2 * (1 - away) + part
        others(lambda j: first(away, part, j).wait_recv())

        def one(o, carry):
            row = (t + o) % 4
            rows = buf[i].reshape(PEERS * 32, 128)
            stage[i, row] = jnp.dot(select[row], rows, preferred_element_type=jnp.float32).astype(BF)
            if away == 0:
                pl.when(o < 4)(lambda: second(away, part, o).start())
            else:
                second(away, part, o).start()
            return carry

        lax.fori_loop(1 - away, 5 - away, one, 0)
        if away == 0:
            recv[part, t, pl.ds(h * K, K)] = stage[i, t]

    chunks(pack)

    mine = [slot == 2 * t + s for s in range(2)]
    ranks = counts_before(mine, source >= 0, before)
    final = sum(jnp.where(mine[s], s * SLOT + 2 * ranks[s], 0) for s in range(2))
    for half in range(2):
        pairs, high, low, top, rest = to_rows([pair, place >> 4, place & 15, final >> 8, final & 255], half)
        notes[1 + 3 * half] = jnp.where(pairs == t, half * K + pol * (K // 2) + high * 16 + low, -1)
        notes[2 + 3 * half] = top
        notes[3 + 3 * half] = rest + pol
    sub = iota((8, 128), 0)
    taller = iota((2 * K, 128), 0)

    def find(b, found):
        one = pl.ds(b, 1)
        for n in (1, 4):
            hit = jnp.where(taller == notes[n, one], 1.0, 0.0).astype(BF)
            known = jnp.where(
                sub == 0, notes[n + 1, one], jnp.where(sub == 1, notes[n + 2, one], jnp.where(sub == 2, 1, 0))
            )
            found = found + lax.dot_general(as_bf16(known), hit, NT, preferred_element_type=jnp.float32)
        return found

    found = lax.fori_loop(0, 8, find, jnp.zeros((8, 2 * K), jnp.float32))
    at = jnp.where(found[2:3] > 0.5, 256.0 * found[0:1] + found[1:2], -1.0).astype(jnp.int32)
    for b in range(6):
        hit = iota((128, 2 * K), 0) == at - b * 128
        merge[b] = jnp.where(hit, 1.0, 0.0).astype(BF)

    def arrived(part, half, row):
        pltpu.make_async_remote_copy(
            stage.at[0, 0], recv.at[part, row, pl.ds(half * K, K)], send2.at[0, 0], recv2.at[part, half * 4 + row],
            device_id=column(half, row), device_id_type=MESH,
        ).wait_recv()

    def finish(n, carry):
        part, row = n // 4, (t + n) % 4
        arrived(part, 1 - h, row)
        pl.when(n % 4 != 0)(lambda: arrived(part, h, row))
        for b in range(6):
            z[part, row, b * 128 : (b + 1) * 128] = jnp.dot(
                merge[b], recv[part, row], preferred_element_type=jnp.float32
            ).astype(BF)
        return carry

    lax.fori_loop(0, 8, finish, 0)

    def sent(away, part):
        others(lambda j: first(away, part, j).wait_send())
        lax.fori_loop(1 - away, 4, lambda o, c: (second(away, part, o).wait_send(), c)[1], 0)

    chunks(sent)


def correlator(number, K):
    def call(voltages, assigned, index):
        return pl.pallas_call(
            functools.partial(correlate, K),
            out_shape=jax.ShapeDtypeStruct((2, 4, 2 * SLOT, 128), BF),
            in_specs=[VMEM, SMEM, ANY],
            out_specs=VMEM,
            scratch_shapes=[
                pltpu.VMEM((2, 16, 2, 2, 32, 128), BF),
                pltpu.VMEM((4, PEERS, 32, 128), BF),
                pltpu.VMEM((4, K, 1024), BF),
                pltpu.VMEM((6, 128, 2 * K), BF),
                pltpu.VMEM((4, 4, K, 128), BF),
                pltpu.VMEM((2, 4, 2 * K, 128), BF),
                pltpu.VMEM((7, 8, 128), jnp.int32),
                pltpu.SemaphoreType.DMA,
                pltpu.SemaphoreType.DMA((4, PEERS)),
                pltpu.SemaphoreType.DMA((4, PEERS)),
                pltpu.SemaphoreType.DMA((4, 4)),
                pltpu.SemaphoreType.DMA((2, 8)),
            ],
            compiler_params=pltpu.CompilerParams(
                collective_id=number, has_side_effects=True, vmem_limit_bytes=48 << 20
            ),
            name=f"gather_{K}",
        )(assigned, index, voltages)

    return call


def gram_kernel(z_ref, out_ref, result, sem):
    def samples(part, s):
        rows = slice(s * SLOT, (s + 1) * SLOT)
        return jnp.concatenate([z_ref[part, b, rows] for b in range(4)], axis=1)

    def times(a, b):
        return lax.dot_general(a, b, NT, preferred_element_type=jnp.float32)

    stores = []
    for s in range(2):
        re, im = samples(0, s), samples(1, s)
        for k in range(2):
            if k == 0:
                both = jnp.concatenate([re, im], axis=1)
                result[s, k] = times(both, both)
            else:
                cross = times(im, re)
                result[s, k] = cross - cross.T
            store = pltpu.make_async_copy(result.at[s, k], out_ref.at[s, 0, k], sem.at[s, k])
            store.start()
            stores.append(store)
    for store in stores:
        store.wait()


def gram(z):
    return pl.pallas_call(
        gram_kernel,
        out_shape=jax.ShapeDtypeStruct((2, 1, 2, SLOT, SLOT), jnp.float32),
        in_specs=[VMEM],
        out_specs=pl.BlockSpec(memory_space=pltpu.HBM),
        scratch_shapes=[pltpu.VMEM((2, 2, SLOT, SLOT), jnp.float32), pltpu.SemaphoreType.DMA((2, 2))],
        name="gram",
    )(z)


def shards(voltages, assignment, slot_subarray_index):
    assigned = assignment.reshape(8, 128)
    level = pl.pallas_call(
        level_kernel,
        out_shape=jax.ShapeDtypeStruct((1,), jnp.int32),
        in_specs=[VMEM, SMEM],
        out_specs=SMEM,
        name="level",
    )(assigned, slot_subarray_index)
    branches = [correlator(number, K) for number, K in enumerate(LEVELS)]
    voltages = voltages.reshape(2, 16, 2, 2, 32, 128)
    return gram(lax.switch(level[0], branches, voltages, assigned, slot_subarray_index))


def solution(mesh):
    placed = (P(None, None, "chan", "tm"), P(), P())
    return jax.shard_map(
        shards,
        mesh=mesh,
        in_specs=placed,
        out_specs=P("tm", "chan", None, None, None),
        check_vma=False,
    )
```

```python
import functools

import jax
import jax.numpy as jnp
from jax import lax
from jax.experimental import pallas as pl
from jax.experimental.pallas import tpu as pltpu
from jax.sharding import PartitionSpec as P

SLOT = 384
LEVELS = (288, 304, 320, 336, 352, 368, 384, 400, 432, 768)
PEERS = 32
SELF = 20
BF = jnp.bfloat16
MESH = pl.DeviceIdType.MESH
NT = (((1,), (1,)), ((), ()))
VMEM = pl.BlockSpec(memory_space=pltpu.VMEM)
SMEM = pl.BlockSpec(memory_space=pltpu.SMEM)
ANY = pl.BlockSpec(memory_space=pl.ANY)


def div(a, b):
    return lax.div(a, jnp.int32(b))


def rem(a, b):
    return lax.rem(a, jnp.int32(b))


def count_dot(a, b):
    return jnp.dot(as_bf16(a), as_bf16(b), preferred_element_type=jnp.float32)


def as_bf16(values):
    return values.astype(jnp.float32).astype(BF)


def iota(shape, dim):
    return lax.broadcasted_iota(jnp.int32, shape, dim)


def slots_of(assigned, index_ref):
    slot = jnp.zeros_like(assigned)
    for s in range(8):
        slot = jnp.where(assigned == index_ref[s], s, slot)
    return slot


def level_kernel(assigned_ref, index_ref, level_ref):
    pair = slots_of(assigned_ref[...], index_ref) >> 1
    half = (iota((8, 128), 1) >> 5) & 1
    most = jnp.int32(0)
    for g in range(4):
        for h in range(2):
            most = jnp.maximum(most, jnp.sum(jnp.where((pair == g) & (half == h), 2, 0)))
    level = jnp.int32(0)
    for rows in LEVELS[:-1]:
        level = level + jnp.where(most > rows, 1, 0)
    level_ref[0] = level


def counts_before(masks, same, before):
    n = len(masks)
    found = count_dot(jnp.concatenate(masks, axis=0), jnp.concatenate([same & before, same], axis=1))
    sub, other = iota((8 * n, 8 * n), 0), iota((8 * n, 8 * n), 1)
    earlier = ((sub >> 3) == (other >> 3)) & (sub > other)
    total = (found[:, :128] + count_dot(earlier, found[:, 128:])).astype(jnp.int32)
    return [total[8 * i : 8 * i + 8] for i in range(n)]


def to_rows(values, half):
    source, target = iota((128, 128), 0), iota((128, 128), 1)
    pick = source == (target >> 6) * 64 + half * 32 + ((target & 63) >> 1)
    moved = count_dot(jnp.concatenate(values, axis=0), pick).astype(jnp.int32)
    return [moved[8 * i : 8 * i + 8] for i in range(len(values))]


def correlate(
    K, assigned_ref, index_ref, v_ref, z, v, buf, select, merge, stage, recv, notes,
    v_sem, send1, recv1, send2, recv2,
):
    chan, t = lax.axis_index("chan"), lax.axis_index("tm")
    xy, h, core = div(chan, 4), rem(div(chan, 2), 2), rem(chan, 2)
    me, depth = xy * 2 + core, h * 4 + t

    def group(j):
        there = rem(div(xy, 4) + 2 + div(j, 8), 4) * 4 + rem(xy + 2 + div(j, 2), 4)
        there_core = rem(core + j, 2)
        return there, there_core, {"chan": (there * 2 + h) * 2 + there_core, "tm": t}

    def others(act):
        def step(j, carry):
            act(j)
            return carry

        lax.fori_loop(0, SELF, step, 0)
        lax.fori_loop(SELF + 1, PEERS, step, 0)

    def column(half, row):
        return {"chan": (xy * 2 + half) * 2 + core, "tm": row}

    load = pltpu.make_async_copy(v_ref, v, v_sem)
    load.start()
    barrier = pltpu.get_barrier_semaphore()

    others(lambda j: pl.semaphore_signal(barrier, inc=1, device_id=group(j)[2], device_id_type=MESH))
    for o in range(1, 8):
        pl.semaphore_signal(
            barrier, inc=1, device_id=column(rem(h + o // 4, 2), rem(t + o, 4)), device_id_type=MESH
        )

    slot = slots_of(assigned_ref[...], index_ref)
    pair = slot >> 1
    source, target = iota((128, 128), 0), iota((128, 128), 1)
    same, before = ((source >> 5) & 1) == ((target >> 5) & 1), source < target
    counts = counts_before([pair == g for g in range(4)], same, before)
    place = sum(jnp.where(pair == g, counts[g], 0) for g in range(4))
    pol = iota((8, 128), 1) & 1
    pairs, high, low = to_rows([pair, place >> 4, place & 15], h)
    notes[0] = pairs * K + pol * (K // 2) + high * 16 + low

    load.wait()
    pl.semaphore_wait(barrier, PEERS - 1 + 7)

    def first(away, part, j):
        there, there_core, device = group(j)
        i = 2 * (1 - away) + part
        return pltpu.make_async_remote_copy(
            v.at[part, there, rem(h + away, 2), there_core], buf.at[i, me], send1.at[i], recv1.at[i],
            device_id=device, device_id_type=MESH,
        )

    def all_first(i):
        every = buf.at[i, pl.ds(0, PEERS - 1)]
        return pltpu.make_async_remote_copy(
            every, every, send1.at[i], recv1.at[i], device_id=group(0)[2], device_id_type=MESH
        )

    def chunks(act):
        for away in (1, 0):

            def step(part, carry, away=away):
                act(away, part)
                return carry

            lax.fori_loop(0, 2, step, 0)

    def start(away, part):
        others(lambda j: first(away, part, j).start())
        buf[2 * (1 - away) + part, me] = v[part, xy, rem(h + away, 2), core]

    chunks(start)

    tall = iota((K, 128), 0)

    def pick(g, carry):
        for b in range(8):
            hit = tall == notes[0, b : b + 1] - g * K
            select[g, :, b * 128 : (b + 1) * 128] = jnp.where(hit, 1.0, 0.0).astype(BF)
        return carry

    lax.fori_loop(0, 4, pick, 0)

    def second(away, part, o):
        i, row = 2 * (1 - away) + part, rem(t + o, 4)
        return pltpu.make_async_remote_copy(
            stage.at[i, row], recv.at[part, t, pl.ds(h * K, K)], send2.at[i], recv2.at[part, depth],
            device_id=column(rem(h + away, 2), row), device_id_type=MESH,
        )

    def pack(away, part):
        i = 2 * (1 - away) + part
        all_first(i).wait_recv()

        def one(o, carry):
            row = rem(t + o, 4)
            rows = buf[i].reshape(PEERS * 32, 128)
            stage[i, row] = jnp.dot(select[row], rows, preferred_element_type=jnp.float32).astype(BF)
            if away == 0:
                pl.when(o < 4)(lambda: second(away, part, o).start())
            else:
                second(away, part, o).start()
            return carry

        lax.fori_loop(1 - away, 5 - away, one, 0)
        if away == 0:
            recv[part, t, pl.ds(h * K, K)] = stage[i, t]

    chunks(pack)

    for i in range(4):
        all_first(i).wait_send()

    mine = [slot == 2 * t + s for s in range(2)]
    ranks = counts_before(mine, source >= 0, before)
    final = sum(jnp.where(mine[s], s * SLOT + 2 * ranks[s], 0) for s in range(2))
    for half in range(2):
        pairs, high, low, top, rest = to_rows([pair, place >> 4, place & 15, final >> 8, final & 255], half)
        notes[1 + 3 * half] = jnp.where(pairs == t, half * K + pol * (K // 2) + high * 16 + low, -1)
        notes[2 + 3 * half] = top
        notes[3 + 3 * half] = rest + pol
    sub = iota((8, 128), 0)
    taller = iota((2 * K, 128), 0)

    def find(b, found):
        one = pl.ds(b, 1)
        for n in (1, 4):
            hit = jnp.where(taller == notes[n, one], 1.0, 0.0).astype(BF)
            known = jnp.where(
                sub == 0, notes[n + 1, one], jnp.where(sub == 1, notes[n + 2, one], jnp.where(sub == 2, 1, 0))
            )
            found = found + lax.dot_general(as_bf16(known), hit, NT, preferred_element_type=jnp.float32)
        return found

    found = lax.fori_loop(0, 8, find, jnp.zeros((8, 2 * K), jnp.float32))
    at = jnp.where(found[2:3] > 0.5, 256.0 * found[0:1] + found[1:2], -1.0).astype(jnp.int32)
    for b in range(6):
        hit = iota((128, 2 * K), 0) == at - b * 128
        merge[b] = jnp.where(hit, 1.0, 0.0).astype(BF)

    def arrived(part, half, row):
        pltpu.make_async_remote_copy(
            stage.at[0, 0], recv.at[part, row, pl.ds(half * K, K)], send2.at[0], recv2.at[part, half * 4 + row],
            device_id=column(half, row), device_id_type=MESH,
        ).wait_recv()

    def finish(n, carry):
        part, row = div(n, 4), rem(t + n, 4)
        arrived(part, 1 - h, row)
        pl.when(rem(n, 4) != 0)(lambda: arrived(part, h, row))
        for b in range(6):
            z[part, row, b * 128 : (b + 1) * 128] = jnp.dot(
                merge[b], recv[part, row], preferred_element_type=jnp.float32
            ).astype(BF)
        return carry

    lax.fori_loop(0, 8, finish, 0)

    def sent(away, part):
        i = 2 * (1 - away) + part
        every = stage.at[i, pl.ds(0, 3 + away)]
        pltpu.make_async_remote_copy(
            every, every, send2.at[i], recv2.at[0, 0], device_id=column(h, rem(t + 1, 4)), device_id_type=MESH
        ).wait_send()

    chunks(sent)


def correlator(number, K):
    def call(voltages, assigned, index):
        return pl.pallas_call(
            functools.partial(correlate, K),
            out_shape=jax.ShapeDtypeStruct((2, 4, 2 * SLOT, 128), BF),
            in_specs=[VMEM, SMEM, ANY],
            out_specs=VMEM,
            scratch_shapes=[
                pltpu.VMEM((2, 16, 2, 2, 32, 128), BF),
                pltpu.VMEM((4, PEERS, 32, 128), BF),
                pltpu.VMEM((4, K, 1024), BF),
                pltpu.VMEM((6, 128, 2 * K), BF),
                pltpu.VMEM((4, 4, K, 128), BF),
                pltpu.VMEM((2, 4, 2 * K, 128), BF),
                pltpu.VMEM((7, 8, 128), jnp.int32),
                pltpu.SemaphoreType.DMA,
                pltpu.SemaphoreType.DMA((4,)),
                pltpu.SemaphoreType.DMA((4,)),
                pltpu.SemaphoreType.DMA((4,)),
                pltpu.SemaphoreType.DMA((2, 8)),
            ],
            compiler_params=pltpu.CompilerParams(
                collective_id=number, has_side_effects=True, vmem_limit_bytes=48 << 20
            ),
            name=f"gather_{K}",
        )(assigned, index, voltages)

    return call


def gram_kernel(z_ref, out_ref, result, sem):
    def samples(part, s):
        rows = slice(s * SLOT, (s + 1) * SLOT)
        return jnp.concatenate([z_ref[part, b, rows] for b in range(4)], axis=1)

    def times(a, b):
        return lax.dot_general(a, b, NT, preferred_element_type=jnp.float32)

    stores = []
    for s in range(2):
        re, im = samples(0, s), samples(1, s)
        for k in range(2):
            if k == 0:
                both = jnp.concatenate([re, im], axis=1)
                result[s, k] = times(both, both)
            else:
                cross = times(im, re)
                result[s, k] = cross - cross.T
            store = pltpu.make_async_copy(result.at[s, k], out_ref.at[s, 0, k], sem.at[s, k])
            store.start()
            stores.append(store)
    for store in stores:
        store.wait()


def gram(z):
    return pl.pallas_call(
        gram_kernel,
        out_shape=jax.ShapeDtypeStruct((2, 1, 2, SLOT, SLOT), jnp.float32),
        in_specs=[VMEM],
        out_specs=pl.BlockSpec(memory_space=pltpu.HBM),
        scratch_shapes=[pltpu.VMEM((2, 2, SLOT, SLOT), jnp.float32), pltpu.SemaphoreType.DMA((2, 2))],
        name="gram",
    )(z)


def shards(voltages, assignment, slot_subarray_index):
    assigned = assignment.reshape(8, 128)
    level = pl.pallas_call(
        level_kernel,
        out_shape=jax.ShapeDtypeStruct((1,), jnp.int32),
        in_specs=[VMEM, SMEM],
        out_specs=SMEM,
        name="level",
    )(assigned, slot_subarray_index)
    branches = [correlator(number, K) for number, K in enumerate(LEVELS)]
    voltages = voltages.reshape(2, 16, 2, 2, 32, 128)
    return gram(lax.switch(level[0], branches, voltages, assigned, slot_subarray_index))


def solution(mesh):
    placed = (P(None, None, "chan", "tm"), P(), P())
    return jax.shard_map(
        shards,
        mesh=mesh,
        in_specs=placed,
        out_specs=P("tm", "chan", None, None, None),
        check_vma=False,
    )
```

```python
import functools

import jax
import jax.numpy as jnp
from jax import lax
from jax.experimental import pallas as pl
from jax.experimental.pallas import tpu as pltpu
from jax.sharding import PartitionSpec as P

SLOT = 384
LEVELS = (288, 304, 320, 336, 352, 368, 384, 400, 432, 768)
PEERS = 32
BF = jnp.bfloat16
MESH = pl.DeviceIdType.MESH
NT = (((1,), (1,)), ((), ()))
VMEM = pl.BlockSpec(memory_space=pltpu.VMEM)
SMEM = pl.BlockSpec(memory_space=pltpu.SMEM)
ANY = pl.BlockSpec(memory_space=pl.ANY)


def div(a, b):
    return lax.div(a, jnp.int32(b))


def rem(a, b):
    return lax.rem(a, jnp.int32(b))


def count_dot(a, b):
    return jnp.dot(as_bf16(a), as_bf16(b), preferred_element_type=jnp.float32)


def as_bf16(values):
    return values.astype(jnp.float32).astype(BF)


def iota(shape, dim):
    return lax.broadcasted_iota(jnp.int32, shape, dim)


def slots_of(assigned, index_ref):
    slot = jnp.zeros_like(assigned)
    for s in range(8):
        slot = jnp.where(assigned == index_ref[s], s, slot)
    return slot


def level_kernel(assigned_ref, index_ref, level_ref):
    pair = slots_of(assigned_ref[...], index_ref) >> 1
    half = (iota((8, 128), 1) >> 5) & 1
    most = jnp.int32(0)
    for g in range(4):
        for h in range(2):
            most = jnp.maximum(most, jnp.sum(jnp.where((pair == g) & (half == h), 2, 0)))
    level = jnp.int32(0)
    for rows in LEVELS[:-1]:
        level = level + jnp.where(most > rows, 1, 0)
    level_ref[0] = level


def counts_before(masks, same, before):
    n = len(masks)
    found = count_dot(jnp.concatenate(masks, axis=0), jnp.concatenate([same & before, same], axis=1))
    sub, other = iota((8 * n, 8 * n), 0), iota((8 * n, 8 * n), 1)
    earlier = ((sub >> 3) == (other >> 3)) & (sub > other)
    total = (found[:, :128] + count_dot(earlier, found[:, 128:])).astype(jnp.int32)
    return [total[8 * i : 8 * i + 8] for i in range(n)]


def to_rows(values, half):
    source, target = iota((128, 128), 0), iota((128, 128), 1)
    pick = source == (target >> 6) * 64 + half * 32 + ((target & 63) >> 1)
    moved = count_dot(jnp.concatenate(values, axis=0), pick).astype(jnp.int32)
    return [moved[8 * i : 8 * i + 8] for i in range(len(values))]


def correlate(
    K, assigned_hbm, index_hbm, v_ref, z, assigned_ref, index_ref, v, buf, select, merge, stage, recv, notes,
    in_sem, send1, recv1, send2, recv2,
):
    chan, t = lax.axis_index("chan"), lax.axis_index("tm")
    xy, h, core = div(chan, 4), rem(div(chan, 2), 2), rem(chan, 2)
    me, depth = xy * 2 + core, h * 4 + t

    x, y = div(xy, 4), rem(xy, 4)

    def group(four, i):
        there = rem(x + 3 - div(four, 2), 4) * 4 + rem(y + 3 - 2 * rem(four, 2) - i // 2, 4)
        there_core = rem(core + 1 - i % 2, 2)
        return there, there_core, {"chan": (there * 2 + h) * 2 + there_core, "tm": t}

    def others(act):
        def step(four, carry):
            for i in range(4):
                act(*group(four, i))
            return carry

        lax.fori_loop(0, PEERS // 4 - 1, step, 0)
        for i in range(3):
            act(*group(jnp.int32(PEERS // 4 - 1), i))

    def column(half, row):
        return {"chan": (xy * 2 + half) * 2 + core, "tm": row}

    loads = [
        pltpu.make_async_copy(source, target, in_sem.at[n])
        for n, (source, target) in enumerate(((assigned_hbm, assigned_ref), (index_hbm, index_ref), (v_ref, v)))
    ]
    for load in loads:
        load.start()
    barrier = pltpu.get_barrier_semaphore()

    for o in (4, 5, 7, 6, 1, 2, 3):
        pl.semaphore_signal(
            barrier, inc=1, device_id=column(rem(h + o // 4, 2), rem(t + o, 4)), device_id_type=MESH
        )
    others(lambda there, there_core, device: pl.semaphore_signal(
        barrier, inc=1, device_id=device, device_id_type=MESH
    ))

    loads[0].wait()
    loads[1].wait()
    slot = slots_of(assigned_ref[...], index_ref)
    pair = slot >> 1
    source, target = iota((128, 128), 0), iota((128, 128), 1)
    same, before = ((source >> 5) & 1) == ((target >> 5) & 1), source < target
    counts = counts_before([pair == g for g in range(4)], same, before)
    place = sum(jnp.where(pair == g, counts[g], 0) for g in range(4))
    pol = iota((8, 128), 1) & 1
    pairs, high, low = to_rows([pair, place >> 4, place & 15], h)
    notes[0] = pairs * K + pol * (K // 2) + high * 16 + low

    loads[2].wait()
    pl.semaphore_wait(barrier, PEERS - 1 + 7)

    def first(away, part, there, there_core, device):
        i = 2 * (1 - away) + part
        return pltpu.make_async_remote_copy(
            v.at[part, there, rem(h + away, 2), there_core], buf.at[i, me], send1.at[i], recv1.at[i],
            device_id=device, device_id_type=MESH,
        )

    def all_first(i):
        every = buf.at[i, pl.ds(0, PEERS - 1)]
        return pltpu.make_async_remote_copy(
            every, every, send1.at[i], recv1.at[i], device_id=group(jnp.int32(0), 0)[2], device_id_type=MESH
        )

    def chunks(act):
        for away in (1, 0):

            def step(part, carry, away=away):
                act(away, part)
                return carry

            lax.fori_loop(0, 2, step, 0)

    def start(away, part):
        others(lambda *peer: first(away, part, *peer).start())
        buf[2 * (1 - away) + part, me] = v[part, xy, rem(h + away, 2), core]

    chunks(start)

    tall = iota((K, 128), 0)

    def pick(g, carry):
        for b in range(8):
            hit = tall == notes[0, b : b + 1] - g * K
            select[g, :, b * 128 : (b + 1) * 128] = jnp.where(hit, 1.0, 0.0).astype(BF)
        return carry

    lax.fori_loop(0, 4, pick, 0)

    def second(away, part, o):
        i, row = 2 * (1 - away) + part, rem(t + o, 4)
        return pltpu.make_async_remote_copy(
            stage.at[i, row], recv.at[part, t, pl.ds(h * K, K)], send2.at[i], recv2.at[part, depth],
            device_id=column(rem(h + away, 2), row), device_id_type=MESH,
        )

    def pack(away, part):
        i = 2 * (1 - away) + part
        all_first(i).wait_recv()

        def one(o, carry):
            row = rem(t + o, 4)
            rows = buf[i].reshape(PEERS * 32, 128)
            stage[i, row] = jnp.dot(select[row], rows, preferred_element_type=jnp.float32).astype(BF)
            if away == 0:
                pl.when(o < 4)(lambda: second(away, part, o).start())
            else:
                second(away, part, o).start()
            return carry

        lax.fori_loop(1 - away, 5 - away, one, 0)
        if away == 0:
            recv[part, t, pl.ds(h * K, K)] = stage[i, t]

    chunks(pack)

    for i in range(4):
        all_first(i).wait_send()

    mine = [slot == 2 * t + s for s in range(2)]
    ranks = counts_before(mine, source >= 0, before)
    final = sum(jnp.where(mine[s], s * SLOT + 2 * ranks[s], 0) for s in range(2))
    for half in range(2):
        pairs, high, low, top, rest = to_rows([pair, place >> 4, place & 15, final >> 8, final & 255], half)
        notes[1 + 3 * half] = jnp.where(pairs == t, half * K + pol * (K // 2) + high * 16 + low, -1)
        notes[2 + 3 * half] = top
        notes[3 + 3 * half] = rest + pol
    sub = iota((8, 128), 0)
    taller = iota((2 * K, 128), 0)

    def find(b, found):
        one = pl.ds(b, 1)
        for n in (1, 4):
            hit = jnp.where(taller == notes[n, one], 1.0, 0.0).astype(BF)
            known = jnp.where(
                sub == 0, notes[n + 1, one], jnp.where(sub == 1, notes[n + 2, one], jnp.where(sub == 2, 1, 0))
            )
            found = found + lax.dot_general(as_bf16(known), hit, NT, preferred_element_type=jnp.float32)
        return found

    found = lax.fori_loop(0, 8, find, jnp.zeros((8, 2 * K), jnp.float32))
    at = jnp.where(found[2:3] > 0.5, 256.0 * found[0:1] + found[1:2], -1.0).astype(jnp.int32)
    for b in range(6):
        hit = iota((128, 2 * K), 0) == at - b * 128
        merge[b] = jnp.where(hit, 1.0, 0.0).astype(BF)

    def arrived(part, half, row):
        pltpu.make_async_remote_copy(
            stage.at[0, 0], recv.at[part, row, pl.ds(half * K, K)], send2.at[0], recv2.at[part, half * 4 + row],
            device_id=column(half, row), device_id_type=MESH,
        ).wait_recv()

    def finish(n, carry):
        part, row = div(n, 4), rem(t + n, 4)
        arrived(part, 1 - h, row)
        pl.when(rem(n, 4) != 0)(lambda: arrived(part, h, row))
        for b in range(6):
            z[part, row, b * 128 : (b + 1) * 128] = jnp.dot(
                merge[b], recv[part, row], preferred_element_type=jnp.float32
            ).astype(BF)
        return carry

    lax.fori_loop(0, 8, finish, 0)

    def sent(away, part):
        i = 2 * (1 - away) + part
        every = stage.at[i, pl.ds(0, 3 + away)]
        pltpu.make_async_remote_copy(
            every, every, send2.at[i], recv2.at[0, 0], device_id=column(h, rem(t + 1, 4)), device_id_type=MESH
        ).wait_send()

    chunks(sent)


def correlator(number, K):
    def call(voltages, assigned, index):
        return pl.pallas_call(
            functools.partial(correlate, K),
            out_shape=jax.ShapeDtypeStruct((2, 4, 2 * SLOT, 128), BF),
            in_specs=[ANY, ANY, ANY],
            out_specs=VMEM,
            scratch_shapes=[
                pltpu.VMEM((8, 128), jnp.int32),
                pltpu.SMEM((8,), jnp.int32),
                pltpu.VMEM((2, 16, 2, 2, 32, 128), BF),
                pltpu.VMEM((4, PEERS, 32, 128), BF),
                pltpu.VMEM((4, K, 1024), BF),
                pltpu.VMEM((6, 128, 2 * K), BF),
                pltpu.VMEM((4, 4, K, 128), BF),
                pltpu.VMEM((2, 4, 2 * K, 128), BF),
                pltpu.VMEM((7, 8, 128), jnp.int32),
                pltpu.SemaphoreType.DMA((3,)),
                pltpu.SemaphoreType.DMA((4,)),
                pltpu.SemaphoreType.DMA((4,)),
                pltpu.SemaphoreType.DMA((4,)),
                pltpu.SemaphoreType.DMA((2, 8)),
            ],
            compiler_params=pltpu.CompilerParams(
                collective_id=number, has_side_effects=True, vmem_limit_bytes=48 << 20
            ),
            name=f"gather_{K}",
        )(assigned, index, voltages)

    return call


def gram_kernel(z_ref, out_ref, result, sem):
    def samples(part, s):
        rows = slice(s * SLOT, (s + 1) * SLOT)
        return jnp.concatenate([z_ref[part, b, rows] for b in range(4)], axis=1)

    def times(a, b):
        return lax.dot_general(a, b, NT, preferred_element_type=jnp.float32)

    stores = []
    for s in range(2):
        re, im = samples(0, s), samples(1, s)
        for k in range(2):
            if k == 0:
                both = jnp.concatenate([re, im], axis=1)
                result[s, k] = times(both, both)
            else:
                cross = times(im, re)
                result[s, k] = cross - cross.T
            store = pltpu.make_async_copy(result.at[s, k], out_ref.at[s, 0, k], sem.at[s, k])
            store.start()
            stores.append(store)
    for store in stores:
        store.wait()


def gram(z):
    return pl.pallas_call(
        gram_kernel,
        out_shape=jax.ShapeDtypeStruct((2, 1, 2, SLOT, SLOT), jnp.float32),
        in_specs=[VMEM],
        out_specs=pl.BlockSpec(memory_space=pltpu.HBM),
        scratch_shapes=[pltpu.VMEM((2, 2, SLOT, SLOT), jnp.float32), pltpu.SemaphoreType.DMA((2, 2))],
        name="gram",
    )(z)


def shards(voltages, assignment, slot_subarray_index):
    assigned = assignment.reshape(8, 128)
    level = pl.pallas_call(
        level_kernel,
        out_shape=jax.ShapeDtypeStruct((1,), jnp.int32),
        in_specs=[VMEM, SMEM],
        out_specs=SMEM,
        name="level",
    )(assigned, slot_subarray_index)
    branches = [correlator(number, K) for number, K in enumerate(LEVELS)]
    voltages = voltages.reshape(2, 16, 2, 2, 32, 128)
    return gram(lax.switch(level[0], branches, voltages, assigned, slot_subarray_index))


def solution(mesh):
    placed = (P(None, None, "chan", "tm"), P(), P())
    return jax.shard_map(
        shards,
        mesh=mesh,
        in_specs=placed,
        out_specs=P("tm", "chan", None, None, None),
        check_vma=False,
    )
```

```python
import functools

import jax
import jax.numpy as jnp
from jax import lax
from jax.experimental import pallas as pl
from jax.experimental.pallas import tpu as pltpu
from jax.sharding import PartitionSpec as P

SLOT = 384
LEVELS = (288, 304, 320, 336, 352, 368, 384, 400, 432, 768)
PEERS = 32
BF = jnp.bfloat16
MESH = pl.DeviceIdType.MESH
NT = (((1,), (1,)), ((), ()))
VMEM = pl.BlockSpec(memory_space=pltpu.VMEM)
SMEM = pl.BlockSpec(memory_space=pltpu.SMEM)
ANY = pl.BlockSpec(memory_space=pl.ANY)


def div(a, b):
    return lax.div(a, jnp.int32(b))


def rem(a, b):
    return lax.rem(a, jnp.int32(b))


def count_dot(a, b):
    return jnp.dot(as_bf16(a), as_bf16(b), preferred_element_type=jnp.float32)


def as_bf16(values):
    return values.astype(jnp.float32).astype(BF)


def iota(shape, dim):
    return lax.broadcasted_iota(jnp.int32, shape, dim)


def slots_of(assigned, index_ref):
    slot = jnp.zeros_like(assigned)
    for s in range(8):
        slot = jnp.where(assigned == index_ref[s], s, slot)
    return slot


def level_kernel(assigned_ref, index_ref, level_ref):
    pair = slots_of(assigned_ref[...], index_ref) >> 1
    half = (iota((8, 128), 1) >> 5) & 1
    most = jnp.int32(0)
    for g in range(4):
        for h in range(2):
            most = jnp.maximum(most, jnp.sum(jnp.where((pair == g) & (half == h), 2, 0)))
    level = jnp.int32(0)
    for rows in LEVELS[:-1]:
        level = level + jnp.where(most > rows, 1, 0)
    level_ref[0] = level


def counts_before(masks, same, before):
    n = len(masks)
    found = count_dot(jnp.concatenate(masks, axis=0), jnp.concatenate([same & before, same], axis=1))
    sub, other = iota((8 * n, 8 * n), 0), iota((8 * n, 8 * n), 1)
    earlier = ((sub >> 3) == (other >> 3)) & (sub > other)
    total = (found[:, :128] + count_dot(earlier, found[:, 128:])).astype(jnp.int32)
    return [total[8 * i : 8 * i + 8] for i in range(n)]


def to_rows(values, half):
    source, target = iota((128, 128), 0), iota((128, 128), 1)
    pick = source == (target >> 6) * 64 + half * 32 + ((target & 63) >> 1)
    moved = count_dot(jnp.concatenate(values, axis=0), pick).astype(jnp.int32)
    return [moved[8 * i : 8 * i + 8] for i in range(len(values))]


def correlate(
    K, assigned_hbm, index_hbm, v_ref, z, assigned_ref, index_ref, v, buf, select, merge, stage, recv, notes,
    in_sem, send1, recv1, send2, recv2,
):
    chan, t = lax.axis_index("chan"), lax.axis_index("tm")
    xy, h, core = div(chan, 4), rem(div(chan, 2), 2), rem(chan, 2)
    me, depth = xy * 2 + core, h * 4 + t

    x, y = div(xy, 4), rem(xy, 4)

    def group(four, i):
        there = rem(x + 3 - div(four, 2), 4) * 4 + rem(y + 3 - 2 * rem(four, 2) - i // 2, 4)
        there_core = rem(core + 1 - i % 2, 2)
        return there, there_core, {"chan": (there * 2 + h) * 2 + there_core, "tm": t}

    def others(act):
        def step(four, carry):
            for i in range(4):
                act(*group(four, i))
            return carry

        lax.fori_loop(0, PEERS // 4 - 1, step, 0)
        for i in range(3):
            act(*group(jnp.int32(PEERS // 4 - 1), i))

    def column(half, row):
        return {"chan": (xy * 2 + half) * 2 + core, "tm": row}

    loads = [
        pltpu.make_async_copy(source, target, in_sem.at[n])
        for n, (source, target) in enumerate(((assigned_hbm, assigned_ref), (index_hbm, index_ref), (v_ref, v)))
    ]
    for load in loads:
        load.start()
    barrier = pltpu.get_barrier_semaphore()

    for o in (4, 5, 7, 6, 1, 2, 3):
        pl.semaphore_signal(
            barrier, inc=1, device_id=column(rem(h + o // 4, 2), rem(t + o, 4)), device_id_type=MESH
        )
    others(lambda there, there_core, device: pl.semaphore_signal(
        barrier, inc=1, device_id=device, device_id_type=MESH
    ))

    loads[0].wait()
    loads[1].wait()
    slot = slots_of(assigned_ref[...], index_ref)
    pair = slot >> 1
    source, target = iota((128, 128), 0), iota((128, 128), 1)
    same, before = ((source >> 5) & 1) == ((target >> 5) & 1), source < target
    counts = counts_before([pair == g for g in range(4)], same, before)
    place = sum(jnp.where(pair == g, counts[g], 0) for g in range(4))
    pol = iota((8, 128), 1) & 1
    pairs, high, low = to_rows([pair, place >> 4, place & 15], h)
    notes[0] = pairs * K + pol * (K // 2) + high * 16 + low

    loads[2].wait()
    pl.semaphore_wait(barrier, PEERS - 1 + 7)

    def first(away, part, there, there_core, device):
        i = 2 * (1 - away) + part
        return pltpu.make_async_remote_copy(
            v.at[part, there, rem(h + away, 2), there_core], buf.at[i, me], send1.at[i], recv1.at[i],
            device_id=device, device_id_type=MESH,
        )

    def all_first(i):
        every = buf.at[i, pl.ds(0, PEERS - 1)]
        return pltpu.make_async_remote_copy(
            every, every, send1.at[i], recv1.at[i], device_id=group(jnp.int32(0), 0)[2], device_id_type=MESH
        )

    def chunks(act):
        for away in (1, 0):

            def step(part, carry, away=away):
                act(away, part)
                return carry

            lax.fori_loop(0, 2, step, 0)

    def start(away, part):
        others(lambda *peer: first(away, part, *peer).start())
        buf[2 * (1 - away) + part, me] = v[part, xy, rem(h + away, 2), core]

    chunks(start)

    tall = iota((K, 128), 0)

    def pick(g, carry):
        for b in range(8):
            hit = tall == notes[0, b : b + 1] - g * K
            select[g, :, b * 128 : (b + 1) * 128] = jnp.where(hit, 1.0, 0.0).astype(BF)
        return carry

    lax.fori_loop(0, 4, pick, 0)

    def second(away, part, o):
        i, row = 2 * (1 - away) + part, rem(t + o, 4)
        return pltpu.make_async_remote_copy(
            stage.at[i, row], recv.at[part, t, pl.ds(h * K, K)], send2.at[i], recv2.at[part, depth],
            device_id=column(rem(h + away, 2), row), device_id_type=MESH,
        )

    def pack(away, part):
        i = 2 * (1 - away) + part
        all_first(i).wait_recv()

        def one(o, carry):
            row = rem(t + o, 4)
            rows = buf[i].reshape(PEERS * 32, 128)
            stage[i, row] = jnp.dot(select[row], rows, preferred_element_type=jnp.float32).astype(BF)
            if away == 0:
                pl.when(o < 4)(lambda: second(away, part, o).start())
            else:
                second(away, part, o).start()
            return carry

        lax.fori_loop(1 - away, 5 - away, one, 0)
        if away == 0:
            recv[part, t, pl.ds(h * K, K)] = stage[i, t]

    chunks(pack)

    for i in range(4):
        all_first(i).wait_send()

    mine = [slot == 2 * t + s for s in range(2)]
    ranks = counts_before(mine, source >= 0, before)
    final = sum(jnp.where(mine[s], s * SLOT + 2 * ranks[s], 0) for s in range(2))
    for half in range(2):
        pairs, high, low, top, rest = to_rows([pair, place >> 4, place & 15, final >> 8, final & 255], half)
        notes[1 + 3 * half] = jnp.where(pairs == t, half * K + pol * (K // 2) + high * 16 + low, -1)
        notes[2 + 3 * half] = top
        notes[3 + 3 * half] = rest + pol
    sub = iota((8, 128), 0)
    taller = iota((2 * K, 128), 0)

    def find(b, found):
        one = pl.ds(b, 1)
        for n in (1, 4):
            hit = jnp.where(taller == notes[n, one], 1.0, 0.0).astype(BF)
            known = jnp.where(
                sub == 0, notes[n + 1, one], jnp.where(sub == 1, notes[n + 2, one], jnp.where(sub == 2, 1, 0))
            )
            found = found + lax.dot_general(as_bf16(known), hit, NT, preferred_element_type=jnp.float32)
        return found

    found = lax.fori_loop(0, 8, find, jnp.zeros((8, 2 * K), jnp.float32))
    at = jnp.where(found[2:3] > 0.5, 256.0 * found[0:1] + found[1:2], -1.0).astype(jnp.int32)
    for b in range(6):
        hit = iota((128, 2 * K), 0) == at - b * 128
        merge[b * 128 : (b + 1) * 128] = jnp.where(hit, 1.0, 0.0).astype(BF)

    def arrived(part, half, row):
        pltpu.make_async_remote_copy(
            stage.at[0, 0], recv.at[part, row, pl.ds(half * K, K)], send2.at[0], recv2.at[part, half * 4 + row],
            device_id=column(half, row), device_id_type=MESH,
        ).wait_recv()

    def finish(n, carry):
        part, pair = div(n, 2), 2 * rem(n, 2)
        blocks = [rem(t + pair + o, 4) for o in range(2)]
        for o in range(2):
            arrived(part, 1 - h, blocks[o])
            if o == 0:
                pl.when(pair != 0)(lambda: arrived(part, h, blocks[0]))
            else:
                arrived(part, h, blocks[1])
        both = jnp.concatenate([recv[part, block] for block in blocks], axis=1)
        placed = jnp.dot(merge[...], both, preferred_element_type=jnp.float32).astype(BF)
        for o in range(2):
            z[part, blocks[o]] = placed[:, o * 128 : (o + 1) * 128]
        return carry

    lax.fori_loop(0, 4, finish, 0)

    def sent(away, part):
        i = 2 * (1 - away) + part
        every = stage.at[i, pl.ds(0, 3 + away)]
        pltpu.make_async_remote_copy(
            every, every, send2.at[i], recv2.at[0, 0], device_id=column(h, rem(t + 1, 4)), device_id_type=MESH
        ).wait_send()

    chunks(sent)


def correlator(number, K):
    def call(voltages, assigned, index):
        return pl.pallas_call(
            functools.partial(correlate, K),
            out_shape=jax.ShapeDtypeStruct((2, 4, 2 * SLOT, 128), BF),
            in_specs=[ANY, ANY, ANY],
            out_specs=VMEM,
            scratch_shapes=[
                pltpu.VMEM((8, 128), jnp.int32),
                pltpu.SMEM((8,), jnp.int32),
                pltpu.VMEM((2, 16, 2, 2, 32, 128), BF),
                pltpu.VMEM((4, PEERS, 32, 128), BF),
                pltpu.VMEM((4, K, 1024), BF),
                pltpu.VMEM((2 * SLOT, 2 * K), BF),
                pltpu.VMEM((4, 4, K, 128), BF),
                pltpu.VMEM((2, 4, 2 * K, 128), BF),
                pltpu.VMEM((7, 8, 128), jnp.int32),
                pltpu.SemaphoreType.DMA((3,)),
                pltpu.SemaphoreType.DMA((4,)),
                pltpu.SemaphoreType.DMA((4,)),
                pltpu.SemaphoreType.DMA((4,)),
                pltpu.SemaphoreType.DMA((2, 8)),
            ],
            compiler_params=pltpu.CompilerParams(
                collective_id=number, has_side_effects=True, vmem_limit_bytes=48 << 20
            ),
            name=f"gather_{K}",
        )(assigned, index, voltages)

    return call


def gram_kernel(z_ref, out_ref, result, sem):
    def samples(part, s):
        rows = slice(s * SLOT, (s + 1) * SLOT)
        return jnp.concatenate([z_ref[part, b, rows] for b in range(4)], axis=1)

    def times(a, b):
        return lax.dot_general(a, b, NT, preferred_element_type=jnp.float32)

    stores = []
    for s in range(2):
        re, im = samples(0, s), samples(1, s)
        for k in range(2):
            if k == 0:
                both = jnp.concatenate([re, im], axis=1)
                result[s, k] = times(both, both)
            else:
                cross = times(im, re)
                result[s, k] = cross - cross.T
            store = pltpu.make_async_copy(result.at[s, k], out_ref.at[s, 0, k], sem.at[s, k])
            store.start()
            stores.append(store)
    for store in stores:
        store.wait()


def gram(z):
    return pl.pallas_call(
        gram_kernel,
        out_shape=jax.ShapeDtypeStruct((2, 1, 2, SLOT, SLOT), jnp.float32),
        in_specs=[VMEM],
        out_specs=pl.BlockSpec(memory_space=pltpu.HBM),
        scratch_shapes=[pltpu.VMEM((2, 2, SLOT, SLOT), jnp.float32), pltpu.SemaphoreType.DMA((2, 2))],
        name="gram",
    )(z)


def shards(voltages, assignment, slot_subarray_index):
    assigned = assignment.reshape(8, 128)
    level = pl.pallas_call(
        level_kernel,
        out_shape=jax.ShapeDtypeStruct((1,), jnp.int32),
        in_specs=[VMEM, SMEM],
        out_specs=SMEM,
        name="level",
    )(assigned, slot_subarray_index)
    branches = [correlator(number, K) for number, K in enumerate(LEVELS)]
    voltages = voltages.reshape(2, 16, 2, 2, 32, 128)
    return gram(lax.switch(level[0], branches, voltages, assigned, slot_subarray_index))


def solution(mesh):
    placed = (P(None, None, "chan", "tm"), P(), P())
    return jax.shard_map(
        shards,
        mesh=mesh,
        in_specs=placed,
        out_specs=P("tm", "chan", None, None, None),
        check_vma=False,
    )
```

```python
import functools

import jax
import jax.numpy as jnp
from jax import lax
from jax.experimental import pallas as pl
from jax.experimental.pallas import tpu as pltpu
from jax.sharding import PartitionSpec as P

SLOT = 384
LEVELS = (288, 304, 320, 336, 352, 368, 384, 400, 432, 768)
PEERS = 32
BF = jnp.bfloat16
MESH = pl.DeviceIdType.MESH
NT = (((1,), (1,)), ((), ()))
VMEM = pl.BlockSpec(memory_space=pltpu.VMEM)
SMEM = pl.BlockSpec(memory_space=pltpu.SMEM)
ANY = pl.BlockSpec(memory_space=pl.ANY)


def div(a, b):
    return lax.div(a, jnp.int32(b))


def rem(a, b):
    return lax.rem(a, jnp.int32(b))


def count_dot(a, b):
    return jnp.dot(as_bf16(a), as_bf16(b), preferred_element_type=jnp.float32)


def as_bf16(values):
    return values.astype(jnp.float32).astype(BF)


def iota(shape, dim):
    return lax.broadcasted_iota(jnp.int32, shape, dim)


def slots_of(assigned, index_ref):
    slot = jnp.zeros_like(assigned)
    for s in range(8):
        slot = jnp.where(assigned == index_ref[s], s, slot)
    return slot


def level_kernel(assigned_ref, index_ref, level_ref):
    pair = slots_of(assigned_ref[...], index_ref) >> 1
    half = (iota((8, 128), 1) >> 5) & 1
    most = jnp.int32(0)
    for g in range(4):
        for h in range(2):
            most = jnp.maximum(most, jnp.sum(jnp.where((pair == g) & (half == h), 2, 0)))
    level = jnp.int32(0)
    for rows in LEVELS[:-1]:
        level = level + jnp.where(most > rows, 1, 0)
    level_ref[0] = level


def counts_before(masks, same, before):
    n = len(masks)
    found = count_dot(jnp.concatenate(masks, axis=0), jnp.concatenate([same & before, same], axis=1))
    sub, other = iota((8 * n, 8 * n), 0), iota((8 * n, 8 * n), 1)
    earlier = ((sub >> 3) == (other >> 3)) & (sub > other)
    total = (found[:, :128] + count_dot(earlier, found[:, 128:])).astype(jnp.int32)
    return [total[8 * i : 8 * i + 8] for i in range(n)]


def to_rows(values, half):
    source, target = iota((128, 128), 0), iota((128, 128), 1)
    pick = source == (target >> 6) * 64 + half * 32 + ((target & 63) >> 1)
    moved = count_dot(jnp.concatenate(values, axis=0), pick).astype(jnp.int32)
    return [moved[8 * i : 8 * i + 8] for i in range(len(values))]


def correlate(
    K, assigned_hbm, index_hbm, v_ref, z, assigned_ref, index_ref, v, buf, select, merge, stage, recv, notes,
    in_sem, send1, recv1, send2, recv2,
):
    chan, t = lax.axis_index("chan"), lax.axis_index("tm")
    xy, h, core = div(chan, 4), rem(div(chan, 2), 2), rem(chan, 2)
    me, depth = xy * 2 + core, h * 4 + t

    x, y = div(xy, 4), rem(xy, 4)

    def group(four, i):
        a, q, s = div(four, 2), rem(four, 2), i // 2
        dx, dy = 2 + a + div(a * (a - 1), 2), 2 + s - q * (1 + 2 * s)
        there = rem(x + dx, 4) * 4 + rem(y + dy, 4)
        there_core = rem(core + 1 - i % 2, 2)
        return there, there_core, {"chan": (there * 2 + h) * 2 + there_core, "tm": t}

    def others(act):
        def step(four, carry):
            for i in range(4):
                act(*group(four, i))
            return carry

        lax.fori_loop(0, PEERS // 4 - 1, step, 0)
        for i in range(3):
            act(*group(jnp.int32(PEERS // 4 - 1), i))

    def column(half, row):
        return {"chan": (xy * 2 + half) * 2 + core, "tm": row}

    loads = [
        pltpu.make_async_copy(source, target, in_sem.at[n])
        for n, (source, target) in enumerate(((assigned_hbm, assigned_ref), (index_hbm, index_ref), (v_ref, v)))
    ]
    for load in loads:
        load.start()
    barrier = pltpu.get_barrier_semaphore()

    for o in (4, 5, 7, 6, 1, 2, 3):
        pl.semaphore_signal(
            barrier, inc=1, device_id=column(rem(h + o // 4, 2), rem(t + o, 4)), device_id_type=MESH
        )
    others(lambda there, there_core, device: pl.semaphore_signal(
        barrier, inc=1, device_id=device, device_id_type=MESH
    ))

    loads[0].wait()
    loads[1].wait()
    slot = slots_of(assigned_ref[...], index_ref)
    pair = slot >> 1
    source, target = iota((128, 128), 0), iota((128, 128), 1)
    same, before = ((source >> 5) & 1) == ((target >> 5) & 1), source < target
    counts = counts_before([pair == g for g in range(4)], same, before)
    place = sum(jnp.where(pair == g, counts[g], 0) for g in range(4))
    pol = iota((8, 128), 1) & 1
    pairs, high, low = to_rows([pair, place >> 4, place & 15], h)
    notes[0] = pairs * K + pol * (K // 2) + high * 16 + low

    loads[2].wait()
    pl.semaphore_wait(barrier, PEERS - 1 + 7)

    def first(away, part, there, there_core, device):
        i = 2 * (1 - away) + part
        return pltpu.make_async_remote_copy(
            v.at[part, there, rem(h + away, 2), there_core], buf.at[i, me], send1.at[i], recv1.at[i],
            device_id=device, device_id_type=MESH,
        )

    def all_first(i):
        every = buf.at[i, pl.ds(0, PEERS - 1)]
        return pltpu.make_async_remote_copy(
            every, every, send1.at[i], recv1.at[i], device_id=group(jnp.int32(0), 0)[2], device_id_type=MESH
        )

    def chunks(act):
        for away in (1, 0):

            def step(part, carry, away=away):
                act(away, part)
                return carry

            lax.fori_loop(0, 2, step, 0)

    def start(away, part):
        others(lambda *peer: first(away, part, *peer).start())
        buf[2 * (1 - away) + part, me] = v[part, xy, rem(h + away, 2), core]

    chunks(start)

    tall = iota((K, 128), 0)

    def pick(g, carry):
        for b in range(8):
            hit = tall == notes[0, b : b + 1] - g * K
            select[g, :, b * 128 : (b + 1) * 128] = jnp.where(hit, 1.0, 0.0).astype(BF)
        return carry

    lax.fori_loop(0, 4, pick, 0)

    def second(away, part, o):
        i, row = 2 * (1 - away) + part, rem(t + o, 4)
        return pltpu.make_async_remote_copy(
            stage.at[i, row], recv.at[part, t, pl.ds(h * K, K)], send2.at[i], recv2.at[part, depth],
            device_id=column(rem(h + away, 2), row), device_id_type=MESH,
        )

    def pack(away, part):
        i = 2 * (1 - away) + part
        all_first(i).wait_recv()

        def one(o, carry):
            row = rem(t + o, 4)
            rows = buf[i].reshape(PEERS * 32, 128)
            stage[i, row] = jnp.dot(select[row], rows, preferred_element_type=jnp.float32).astype(BF)
            if away == 0:
                pl.when(o < 4)(lambda: second(away, part, o).start())
            else:
                second(away, part, o).start()
            return carry

        lax.fori_loop(1 - away, 5 - away, one, 0)
        if away == 0:
            recv[part, t, pl.ds(h * K, K)] = stage[i, t]

    chunks(pack)

    for i in range(4):
        all_first(i).wait_send()

    mine = [slot == 2 * t + s for s in range(2)]
    ranks = counts_before(mine, source >= 0, before)
    final = sum(jnp.where(mine[s], s * SLOT + 2 * ranks[s], 0) for s in range(2))
    for half in range(2):
        pairs, high, low, top, rest = to_rows([pair, place >> 4, place & 15, final >> 8, final & 255], half)
        notes[1 + 3 * half] = jnp.where(pairs == t, half * K + pol * (K // 2) + high * 16 + low, -1)
        notes[2 + 3 * half] = top
        notes[3 + 3 * half] = rest + pol
    sub = iota((8, 128), 0)
    taller = iota((2 * K, 128), 0)

    def find(b, found):
        one = pl.ds(b, 1)
        for n in (1, 4):
            hit = jnp.where(taller == notes[n, one], 1.0, 0.0).astype(BF)
            known = jnp.where(
                sub == 0, notes[n + 1, one], jnp.where(sub == 1, notes[n + 2, one], jnp.where(sub == 2, 1, 0))
            )
            found = found + lax.dot_general(as_bf16(known), hit, NT, preferred_element_type=jnp.float32)
        return found

    found = lax.fori_loop(0, 8, find, jnp.zeros((8, 2 * K), jnp.float32))
    at = jnp.where(found[2:3] > 0.5, 256.0 * found[0:1] + found[1:2], -1.0).astype(jnp.int32)
    for b in range(6):
        hit = iota((128, 2 * K), 0) == at - b * 128
        merge[b * 128 : (b + 1) * 128] = jnp.where(hit, 1.0, 0.0).astype(BF)

    def arrived(part, half, row):
        pltpu.make_async_remote_copy(
            stage.at[0, 0], recv.at[part, row, pl.ds(half * K, K)], send2.at[0], recv2.at[part, half * 4 + row],
            device_id=column(half, row), device_id_type=MESH,
        ).wait_recv()

    def finish(n, carry):
        part, pair = div(n, 2), 2 * rem(n, 2)
        blocks = [rem(t + pair + o, 4) for o in range(2)]
        for o in range(2):
            arrived(part, 1 - h, blocks[o])
            if o == 0:
                pl.when(pair != 0)(lambda: arrived(part, h, blocks[0]))
            else:
                arrived(part, h, blocks[1])
        both = jnp.concatenate([recv[part, block] for block in blocks], axis=1)
        placed = jnp.dot(merge[...], both, preferred_element_type=jnp.float32).astype(BF)
        for o in range(2):
            z[part, blocks[o]] = placed[:, o * 128 : (o + 1) * 128]
        return carry

    lax.fori_loop(0, 4, finish, 0)

    def sent(away, part):
        i = 2 * (1 - away) + part
        every = stage.at[i, pl.ds(0, 3 + away)]
        pltpu.make_async_remote_copy(
            every, every, send2.at[i], recv2.at[0, 0], device_id=column(h, rem(t + 1, 4)), device_id_type=MESH
        ).wait_send()

    chunks(sent)


def correlator(number, K):
    def call(voltages, assigned, index):
        return pl.pallas_call(
            functools.partial(correlate, K),
            out_shape=jax.ShapeDtypeStruct((2, 4, 2 * SLOT, 128), BF),
            in_specs=[ANY, ANY, ANY],
            out_specs=VMEM,
            scratch_shapes=[
                pltpu.VMEM((8, 128), jnp.int32),
                pltpu.SMEM((8,), jnp.int32),
                pltpu.VMEM((2, 16, 2, 2, 32, 128), BF),
                pltpu.VMEM((4, PEERS, 32, 128), BF),
                pltpu.VMEM((4, K, 1024), BF),
                pltpu.VMEM((2 * SLOT, 2 * K), BF),
                pltpu.VMEM((4, 4, K, 128), BF),
                pltpu.VMEM((2, 4, 2 * K, 128), BF),
                pltpu.VMEM((7, 8, 128), jnp.int32),
                pltpu.SemaphoreType.DMA((3,)),
                pltpu.SemaphoreType.DMA((4,)),
                pltpu.SemaphoreType.DMA((4,)),
                pltpu.SemaphoreType.DMA((4,)),
                pltpu.SemaphoreType.DMA((2, 8)),
            ],
            compiler_params=pltpu.CompilerParams(
                collective_id=number, has_side_effects=True, vmem_limit_bytes=48 << 20
            ),
            name=f"gather_{K}",
        )(assigned, index, voltages)

    return call


def gram_kernel(z_ref, out_ref, result, sem):
    def samples(part, s):
        rows = slice(s * SLOT, (s + 1) * SLOT)
        return jnp.concatenate([z_ref[part, b, rows] for b in range(4)], axis=1)

    def times(a, b):
        return lax.dot_general(a, b, NT, preferred_element_type=jnp.float32)

    stores = []
    for s in range(2):
        re, im = samples(0, s), samples(1, s)
        for k in range(2):
            if k == 0:
                both = jnp.concatenate([re, im], axis=1)
                result[s, k] = times(both, both)
            else:
                cross = times(im, re)
                result[s, k] = cross - cross.T
            store = pltpu.make_async_copy(result.at[s, k], out_ref.at[s, 0, k], sem.at[s, k])
            store.start()
            stores.append(store)
    for store in stores:
        store.wait()


def gram(z):
    return pl.pallas_call(
        gram_kernel,
        out_shape=jax.ShapeDtypeStruct((2, 1, 2, SLOT, SLOT), jnp.float32),
        in_specs=[VMEM],
        out_specs=pl.BlockSpec(memory_space=pltpu.HBM),
        scratch_shapes=[pltpu.VMEM((2, 2, SLOT, SLOT), jnp.float32), pltpu.SemaphoreType.DMA((2, 2))],
        name="gram",
    )(z)


def shards(voltages, assignment, slot_subarray_index):
    assigned = assignment.reshape(8, 128)
    level = pl.pallas_call(
        level_kernel,
        out_shape=jax.ShapeDtypeStruct((1,), jnp.int32),
        in_specs=[VMEM, SMEM],
        out_specs=SMEM,
        name="level",
    )(assigned, slot_subarray_index)
    branches = [correlator(number, K) for number, K in enumerate(LEVELS)]
    voltages = voltages.reshape(2, 16, 2, 2, 32, 128)
    return gram(lax.switch(level[0], branches, voltages, assigned, slot_subarray_index))


def solution(mesh):
    placed = (P(None, None, "chan", "tm"), P(), P())
    return jax.shard_map(
        shards,
        mesh=mesh,
        in_specs=placed,
        out_specs=P("tm", "chan", None, None, None),
        check_vma=False,
    )
```
